32 devices in a mesh: replica: 4 (over y, z), dp: 8 (over x, core).
Axes of the slice: x: 4, y: 2, z: 2, core: 2. Of those that a mesh axis runs over, the one named last changes fastest.
The devices are a block of a 4x4x8 slice.
Arguments:
- x: bfloat16 [2048, 896], P(('replica', 'dp')), parts along dimension 0
- lengths: int32 [2048], P(('replica', 'dp')), parts along dimension 0
- cache: bfloat16 [2, 2048, 64, 576], P(None, ('replica', 'dp')), parts along dimension 1
- w_q: bfloat16 [2, 896, 4608], replicated
- w_o: bfloat16 [2, 4096, 896], replicated
- expert_ids: int32 [2, 2048, 8], P(None, ('replica', 'dp')), parts along dimension 1
- slots: int32 [2, 2048, 8], P(None, ('replica', 'dp')), parts along dimension 1
- route_w: float32 [2, 2048, 8], P(None, ('replica', 'dp')), parts along dimension 1
- w1_exp: bfloat16 [2, 384, 896, 256], P(None, 'dp')
- w3_exp: bfloat16 [2, 384, 896, 256], P(None, 'dp')
- w2_exp: bfloat16 [2, 384, 256, 896], P(None, 'dp')
- w1_sh: bfloat16 [2, 896, 256], P(None, None, 'dp')
- w3_sh: bfloat16 [2, 896, 256], P(None, None, 'dp')
- w2_sh: bfloat16 [2, 256, 896], P(None, 'dp')
Outputs:
- output: bfloat16 [2048, 896], P(('replica', 'dp')), parts along dimension 0
There are 4 independent parts. The reference program is written for one: setup_inputs(seed, part) draws one part's arguments, and reference() takes and returns one part's arrays. A program takes and returns all parts, laid end to end along the dimension named above; an argument that names none is the same for every part.
All inputs are finite; a program needn't handle non-finite values.
Results may differ from the reference program's by a relative error of at most 0.02.
Values are sent between devices in bfloat16 or wider.
A program may use at most 768 MiB of HBM per device.

```python
import jax
import jax.numpy as jnp
from jax import lax

GROUP_SIZE = 8
BATCH_DEV = 64
SEQ_LEN = 64
D_MODEL = 896
NUM_HEADS = 8
EXPERTS = 384
TOP_K = 8
FF_EXPERT = 256
FF_SHARED = 256
CAPACITY = 2
LAYERS = 2
LATENT = 512
ROPE_DIM = 64

KV_DIM = LATENT + ROPE_DIM
TOKENS = GROUP_SIZE * BATCH_DEV
BUFFER_ROWS = EXPERTS * GROUP_SIZE * CAPACITY
ATT_SCALE = 1.0 / (192.0 ** 0.5)
NORM_EPS = 1e-6


def scaled_normal(key, shape, scale):
    return (jax.random.normal(key, shape, jnp.float32) * scale).astype(jnp.bfloat16)


def draw_routing(key):
    key_bias, key_score, key_hot = jax.random.split(key, 3)
    expert_bias = jax.random.randint(key_bias, (LAYERS, 1, EXPERTS), 0, 512)
    raw_score = jax.random.randint(key_score, (LAYERS, TOKENS, EXPERTS), 0, 1024) + expert_bias
    hot_expert = jax.random.randint(key_hot, (LAYERS, GROUP_SIZE, 1, 1), 0, EXPERTS)
    first_rows = jnp.arange(BATCH_DEV)[None, None, :, None] < CAPACITY
    forced = jnp.logical_and(first_rows, jnp.arange(EXPERTS)[None, None, None, :] == hot_expert)
    raw_score = raw_score + 4096 * forced.astype(jnp.int32).reshape(LAYERS, TOKENS, EXPERTS)
    ranked = raw_score * EXPERTS + jnp.arange(EXPERTS)
    expert_ids = lax.top_k(ranked, TOP_K)[1].astype(jnp.int32)
    member = (expert_ids[:, :, :, None] == jnp.arange(EXPERTS)).astype(jnp.int32)
    member = member.reshape(LAYERS, GROUP_SIZE, BATCH_DEV * TOP_K, EXPERTS)
    slot_rank = jnp.sum(jnp.cumsum(member, axis=2) * member, axis=-1) - 1
    slot_rank = slot_rank.reshape(LAYERS, TOKENS, TOP_K)
    slots = jnp.where(slot_rank < CAPACITY, slot_rank, -1).astype(jnp.int32)
    return expert_ids, slots


def setup_inputs(seed: int = 0, part: int = 0) -> dict:
    part_keys = jax.random.split(jax.random.fold_in(jax.random.key(seed), part), 5)
    weight_keys = jax.random.split(jax.random.key(seed + 1), 8)
    x = scaled_normal(part_keys[0], (TOKENS, D_MODEL), 1.0)
    lengths = jax.random.randint(part_keys[1], (TOKENS,), 1, SEQ_LEN + 1).at[0].set(SEQ_LEN).astype(jnp.int32)
    cache = scaled_normal(part_keys[2], (LAYERS, TOKENS, SEQ_LEN, KV_DIM), 1.0)
    expert_ids, slots = draw_routing(part_keys[3])
    route_w = jax.random.uniform(part_keys[4], (LAYERS, TOKENS, TOP_K), jnp.float32, 0.5, 1.5) * (3.0 / TOP_K)
    return dict(
        x=x,
        lengths=lengths,
        cache=cache,
        w_q=scaled_normal(weight_keys[0], (LAYERS, D_MODEL, NUM_HEADS * KV_DIM), 1.5 * D_MODEL ** -0.5),
        w_o=scaled_normal(weight_keys[1], (LAYERS, NUM_HEADS * LATENT, D_MODEL), (NUM_HEADS * LATENT) ** -0.5),
        expert_ids=expert_ids,
        slots=slots,
        route_w=route_w,
        w1_exp=scaled_normal(weight_keys[2], (LAYERS, EXPERTS, D_MODEL, FF_EXPERT), D_MODEL ** -0.5),
        w3_exp=scaled_normal(weight_keys[3], (LAYERS, EXPERTS, D_MODEL, FF_EXPERT), D_MODEL ** -0.5),
        w2_exp=scaled_normal(weight_keys[4], (LAYERS, EXPERTS, FF_EXPERT, D_MODEL), 1.5 * FF_EXPERT ** -0.5),
        w1_sh=scaled_normal(weight_keys[5], (LAYERS, D_MODEL, FF_SHARED), D_MODEL ** -0.5),
        w3_sh=scaled_normal(weight_keys[6], (LAYERS, D_MODEL, FF_SHARED), D_MODEL ** -0.5),
        w2_sh=scaled_normal(weight_keys[7], (LAYERS, FF_SHARED, D_MODEL), 2.0 * FF_SHARED ** -0.5),
    )


def rms_norm(values):
    vals32 = values.astype(jnp.float32)
    return vals32 * lax.rsqrt(jnp.mean(vals32 * vals32, axis=-1, keepdims=True) + NORM_EPS)


def attend_block(block_args):
    q_block, cache_block, len_block = block_args
    scores = jnp.einsum('bhc,btc->bht', q_block.astype(jnp.float32), cache_block.astype(jnp.float32)) * ATT_SCALE
    valid = jnp.arange(SEQ_LEN)[None, None, :] < len_block[:, None, None]
    probs = jax.nn.softmax(jnp.where(valid, scores, -jnp.inf), axis=-1)
    probs = probs.astype(jnp.bfloat16).astype(jnp.float32)
    return jnp.einsum('bht,btc->bhc', probs, cache_block[:, :, :LATENT].astype(jnp.float32))


def reference(x, lengths, cache, w_q, w_o, expert_ids, slots, route_w, w1_exp, w3_exp, w2_exp, w1_sh, w3_sh, w2_sh):
    owner_dev = jnp.arange(TOKENS) // BATCH_DEV
    len_blocks = lengths.reshape(GROUP_SIZE, BATCH_DEV)

    def layer_step(resid, layer_args):
        cache_l, w_q_l, w_o_l, ids_l, slot_l, gate_w, w1_e, w3_e, w2_e, w1_s, w3_s, w2_s = layer_args
        normed = rms_norm(resid).astype(jnp.bfloat16)
        queries = jnp.dot(normed, w_q_l, preferred_element_type=jnp.float32).astype(jnp.bfloat16)
        queries = queries.reshape(GROUP_SIZE, BATCH_DEV, NUM_HEADS, KV_DIM)
        attn = lax.map(attend_block, (queries, cache_l.reshape(GROUP_SIZE, BATCH_DEV, SEQ_LEN, KV_DIM), len_blocks))
        attn = attn.astype(jnp.bfloat16).reshape(TOKENS, NUM_HEADS * LATENT)
        resid = (resid.astype(jnp.float32) + jnp.dot(attn, w_o_l, preferred_element_type=jnp.float32)).astype(jnp.bfloat16)
        ffn_in = rms_norm(resid).astype(jnp.bfloat16)
        shared_gate = jnp.dot(ffn_in, w3_s, preferred_element_type=jnp.float32)
        shared_up = jnp.dot(ffn_in, w1_s, preferred_element_type=jnp.float32)
        shared_h = (jax.nn.silu(shared_gate) * shared_up).astype(jnp.bfloat16)
        shared_out = jnp.dot(shared_h, w2_s, preferred_element_type=jnp.float32)
        buf_rows = jnp.where(slot_l >= 0, ids_l * (GROUP_SIZE * CAPACITY) + owner_dev[:, None] * CAPACITY + slot_l, BUFFER_ROWS)
        copies = jnp.broadcast_to(ffn_in[:, None, :], (TOKENS, TOP_K, D_MODEL)).reshape(TOKENS * TOP_K, D_MODEL)
        buffer = jnp.zeros((BUFFER_ROWS, D_MODEL), jnp.bfloat16).at[buf_rows.reshape(-1)].set(copies, mode='drop')
        buffer = buffer.reshape(EXPERTS, GROUP_SIZE * CAPACITY, D_MODEL).astype(jnp.float32)
        gate_in = jnp.einsum('ecd,edf->ecf', buffer, w3_e.astype(jnp.float32))
        up_in = jnp.einsum('ecd,edf->ecf', buffer, w1_e.astype(jnp.float32))
        hidden = (jax.nn.silu(gate_in) * up_in).astype(jnp.bfloat16).astype(jnp.float32)
        expert_out = jnp.einsum('ecf,efd->ecd', hidden, w2_e.astype(jnp.float32)).astype(jnp.bfloat16)
        picked = jnp.take(expert_out.reshape(BUFFER_ROWS, D_MODEL), buf_rows, axis=0, mode='fill', fill_value=0)
        routed = jnp.sum(gate_w[:, :, None] * picked.astype(jnp.float32), axis=1)
        resid = (resid.astype(jnp.float32) + routed + shared_out).astype(jnp.bfloat16)
        return resid, None

    final_x = lax.scan(layer_step, x, (cache, w_q, w_o, expert_ids, slots, route_w, w1_exp, w3_exp, w2_exp, w1_sh, w3_sh, w2_sh))[0]
    return final_x
```

```python
import functools

import jax
import jax.numpy as jnp
from jax import lax
from jax.experimental import pallas as pl
from jax.experimental.pallas import tpu as pltpu
from jax.sharding import PartitionSpec as P

NORM_EPS = 1e-6
ATT_SCALE = 1.0 / (192.0 ** 0.5)
LATENT = 512
TB = 16
GA = 4
NS = 4
GB = 8
DROPPED = -(1 << 20)
F32 = jnp.float32
BF16 = jnp.bfloat16


def rms_norm(v):
    return v * lax.rsqrt(jnp.mean(v * v, axis=-1, keepdims=True) + NORM_EPS)


def dot(a, b):
    return jnp.dot(a, b, preferred_element_type=F32)


def dot_nt(a, b):
    return lax.dot_general(a, b, (((1,), (1,)), ((), ())), preferred_element_type=F32)


def make_kernel(group, layers, tok, d_model, seq, kv_dim, heads, n_exp, top_k, cap, ff, chunks):
    chips = group // 2
    rows_e = group * cap
    n_rows = n_exp * rows_e
    n_tok = group * tok
    n_bg = tok // TB
    n_a = n_exp // GA
    n_b = n_exp // GB
    pair = 2 * kv_dim

    def kernel(x_ref, len_ref, tab_ref, w1s_ref, w3s_ref, w2s_ref, cache_hbm, wq_hbm, wo_hbm, w1_hbm, w3_hbm, w2_hbm,
               out_ref,
               wqb, wob, kvb, w1b, w3b, w2b, xres, qs, os, g_all, tabs, disp, comb, xd, hid, hsb, pf,
               psend, prx, fsend, frx, n1send, n1rx, n2send, n2rx,
               wq_sem, kv_sem, wo_sem, w13_sem, w2_sem, tab_s, tab_r, ag_s, ag_r, rs_s, rs_r):
        me = lax.axis_index("dp")
        c = lax.rem(me, 2)
        xx = me // 2
        fwd_chip = lax.rem(xx + 1 + 2 * c, chips)
        bwd_chip = lax.rem(xx + 3 - 2 * c, chips)
        far_chip = lax.rem(xx + 2, chips)
        fwd = 2 * fwd_chip + c
        bwd = 2 * bwd_chip + c
        far = 2 * far_chip + c
        partner = 2 * xx + 1 - c

        def wq_copy(l, p):
            return pltpu.make_async_copy(wq_hbm.at[l, :, pl.ds(p * pair, pair)], wqb.at[:, pl.ds(p * pair, pair)], wq_sem.at[p])

        def kv_copy(l, b):
            return pltpu.make_async_copy(cache_hbm.at[l, pl.ds(b * TB, TB)], kvb.at[pl.ds(b * TB, TB)], kv_sem.at[b])

        def wo_copy(l):
            return pltpu.make_async_copy(wo_hbm.at[l], wob, wo_sem)

        def w13_copies(l, i):
            slot = lax.rem(i, NS)
            return (pltpu.make_async_copy(w1_hbm.at[l, pl.ds(i * GA, GA)], w1b.at[slot], w13_sem.at[0, slot]),
                    pltpu.make_async_copy(w3_hbm.at[l, pl.ds(i * GA, GA)], w3b.at[slot], w13_sem.at[1, slot]))

        def w2_copy(l, k, i):
            c0, cw = chunks[k]
            return pltpu.make_async_copy(w2_hbm.at[l, pl.ds(i * GB, GB), :, pl.ds(c0, cw)],
                                         w2b.at[i, :, :, pl.ds(0, cw)], w2_sem.at[i])

        def start_attn(l):
            for p in range(heads // 2):
                wq_copy(l, p).start()
            for b in range(n_bg):
                kv_copy(l, b).start()
            wo_copy(l).start()

        def start_w13(l, i):
            for cp in w13_copies(l, i):
                cp.start()

        start_attn(0)

        barrier = pltpu.get_barrier_semaphore()
        for o in range(1, group):
            pl.semaphore_signal(barrier, inc=1, device_id={"dp": lax.rem(me + o, group)}, device_id_type=pl.DeviceIdType.MESH)
        pl.semaphore_wait(barrier, group - 1)

        def remote(src, dst, s_sem, r_sem, dev):
            return pltpu.make_async_remote_copy(src_ref=src, dst_ref=dst, send_sem=s_sem, recv_sem=r_sem,
                                                device_id={"dp": dev}, device_id_type=pl.DeviceIdType.MESH)

        tab_cps = []
        for o in range(1, group):
            cp = remote(tab_ref, tabs.at[me], tab_s.at[o - 1], tab_r.at[o - 1], lax.rem(me + o, group))
            cp.start()
            tab_cps.append(cp)
        tabs[me] = tab_ref[...]

        pending_sends = list(tab_cps)

        for l in range(layers):
            x_in = x_ref[...] if l == 0 else xres[...]
            h = rms_norm(x_in.astype(F32)).astype(BF16)
            for p in range(heads // 2):
                wq_copy(l, p).wait()
                qp = dot(h, wqb[:, p * pair:(p + 1) * pair])
                lo = (kv_dim // 128) * 128
                odd = pltpu.roll(qp[:, lo:], pair - kv_dim, 1)[:, :kv_dim].astype(BF16)
                even = qp[:, :kv_dim].astype(BF16)
                for b in range(n_bg):
                    qs[b, (2 * p) * TB:(2 * p + 1) * TB, :] = even[b * TB:(b + 1) * TB]
                    qs[b, (2 * p + 1) * TB:(2 * p + 2) * TB, :] = odd[b * TB:(b + 1) * TB]
            if l == 0:
                for i in range(2):
                    start_w13(0, i)
            for b in range(n_bg):
                kv_copy(l, b).wait()
            cols = TB * seq
            row_i = lax.broadcasted_iota(jnp.int32, (heads * TB, cols), 0)
            col_i = lax.broadcasted_iota(jnp.int32, (heads * TB, cols), 1)
            own = lax.rem(row_i, TB) == col_i // seq
            lane = lax.broadcasted_iota(jnp.int32, (1, cols), 1)
            for b in range(n_bg):
                lim = jnp.zeros((1, cols), jnp.int32)
                for i in range(TB):
                    lim = jnp.where(lane // seq == i, len_ref[b * TB + i], lim)
                in_len = lax.rem(lane, seq) < lim
                keys = kvb[b * TB:(b + 1) * TB].reshape(cols, kv_dim)
                s = dot_nt(qs[b], keys) * ATT_SCALE
                s = jnp.where(jnp.logical_and(own, in_len), s, -jnp.inf)
                e = jnp.exp(s - jnp.max(s, axis=-1, keepdims=True))
                pr = (e * (1.0 / jnp.sum(e, axis=-1, keepdims=True))).astype(BF16)
                vals = kvb[b * TB:(b + 1) * TB, :, :LATENT].reshape(cols, LATENT)
                o_blk = dot(pr, vals).astype(BF16)
                for hh in range(heads):
                    os[b * TB:(b + 1) * TB, hh * LATENT:(hh + 1) * LATENT] = o_blk[hh * TB:(hh + 1) * TB]
            if l == 0:
                for i in range(2, NS):
                    start_w13(0, i)
                for i in range(n_b):
                    w2_copy(0, 0, i).start()
            wo_copy(l).wait()
            x1 = (x_in.astype(F32) + dot(os[...], wob[...])).astype(BF16)
            xres[...] = x1
            g_all[l, me] = rms_norm(x1.astype(F32)).astype(BF16)

            def ag(k, blk, dev):
                cp = remote(g_all.at[l, blk], g_all.at[l, blk], ag_s.at[l, k], ag_r.at[l, k], dev)
                cp.start()
                pending_sends.append(cp)
                return cp

            cp_a = ag(0, me, fwd)
            cp_b = ag(1, me, bwd)
            cp_d0 = ag(2, me, partner)

            if l == 0:
                for cp in tab_cps:
                    cp.wait_recv()
            base = (me * n_rows).astype(F32)
            half = lax.broadcasted_iota(jnp.int32, (2 * top_k, 2 * tok), 1) < tok
            tiles = []
            for ch in range(chips):
                t = jnp.where(half, tabs[2 * ch, 2 * top_k * l:2 * top_k * (l + 1)],
                              tabs[2 * ch + 1, 2 * top_k * l:2 * top_k * (l + 1)])
                tiles.append(t)
            codes = [(t[:top_k] - base).astype(jnp.int32) for t in tiles]
            codes = jnp.concatenate(codes, axis=1)

            def build_disp(i, _):
                r0 = pl.multiple_of(i * 32, 32)
                ri = lax.broadcasted_iota(jnp.int32, (32, n_tok), 0) + r0
                hit = jnp.zeros((32, n_tok), F32)
                for j in range(top_k):
                    hit = jnp.where(ri == codes[j:j + 1, :], 1.0, hit)
                disp[pl.ds(r0, 32), :] = hit.astype(BF16)
                return 0

            lax.fori_loop(0, n_rows // 32, build_disp, 0)
            for ch in range(chips):
                tt = tiles[ch].T
                tcode = (tt[:, :top_k] - base).astype(jnp.int32)
                tw = tt[:, top_k:2 * top_k]
                for rb in range(n_rows // 128):
                    ri = lax.broadcasted_iota(jnp.int32, (2 * tok, 128), 1) + rb * 128
                    w = jnp.zeros((2 * tok, 128), F32)
                    for j in range(top_k):
                        w = jnp.where(ri == tcode[:, j:j + 1], tw[:, j:j + 1], w)
                    w_hi = w.astype(BF16)
                    rem1 = w - w_hi.astype(F32)
                    w_mid = rem1.astype(BF16)
                    w_lo = (rem1 - w_mid.astype(F32)).astype(BF16)
                    sl = slice(rb * 128, (rb + 1) * 128)
                    comb[ch, 0:2 * tok, sl] = w_hi
                    comb[ch, 2 * tok:4 * tok, sl] = w_mid
                    comb[ch, 4 * tok:6 * tok, sl] = w_lo

            cp_a.wait_recv()
            cp_f = ag(3, bwd, fwd)
            cp_d1 = ag(4, bwd, partner)
            cp_b.wait_recv()
            cp_d2 = ag(5, fwd, partner)
            cp_f.wait_recv()
            cp_d3 = ag(6, far, partner)
            for cp in (cp_d0, cp_d1, cp_d2, cp_d3):
                cp.wait_recv()

            g_mat = g_all[l].reshape(n_tok, d_model)
            s_gate = dot_nt(g_mat, w3s_ref[l])
            s_up = dot_nt(g_mat, w1s_ref[l])
            hsb[...] = (s_gate * jax.nn.sigmoid(s_gate) * s_up).astype(BF16)

            def dispatch(i, _):
                r0 = pl.multiple_of(i * 256, 256)
                xd[pl.ds(r0, 256), :] = dot(disp[pl.ds(r0, 256), :], g_all[l].reshape(n_tok, d_model)).astype(BF16)
                return 0

            lax.fori_loop(0, n_rows // 256, dispatch, 0)

            def step_a(i, _):
                slot = lax.rem(i, NS)
                for cp in w13_copies(l, i):
                    cp.wait()
                for k in range(GA):
                    r0 = pl.multiple_of((i * GA + k) * rows_e, rows_e)
                    xe = xd[pl.ds(r0, rows_e), :]
                    gate = dot(xe, w3b[slot, k])
                    up = dot(xe, w1b[slot, k])
                    hid[pl.ds(r0, rows_e), :] = (gate * jax.nn.sigmoid(gate) * up).astype(BF16)

                @pl.when(i + NS < n_a)
                def _():
                    start_w13(l, i + NS)

                if l + 1 < layers:
                    @pl.when(i + NS >= n_a)
                    def _():
                        start_w13(l + 1, i + NS - n_a)
                return 0

            lax.fori_loop(0, n_a, step_a, 0)

            def step_b(k):
                cw = chunks[k][1]

                def body(i, _):
                    w2_copy(l, k, i).wait()
                    for kk in range(GB):
                        r0 = pl.multiple_of((i * GB + kk) * rows_e, rows_e)
                        xd[pl.ds(r0, rows_e), 0:cw] = dot(hid[pl.ds(r0, rows_e), :], w2b[i, kk, :, 0:cw]).astype(BF16)
                    if k + 1 < len(chunks):
                        w2_copy(l, k + 1, i).start()
                    elif l + 1 < layers:
                        w2_copy(l + 1, 0, i).start()
                    return 0

                return body

            def combine(k):
                c0, cw = chunks[k]
                cs = slice(c0, c0 + cw)
                for ch in range(chips):
                    r = dot(comb[ch], xd[:, 0:cw])
                    sh = dot(hsb[ch * 2 * tok:(ch + 1) * 2 * tok, :], w2s_ref[l, :, cs])
                    r = sh + (r[0:2 * tok] + r[2 * tok:4 * tok] + r[4 * tok:6 * tok])
                    pf[2 * ch, :, cs] = r[:tok]
                    pf[2 * ch + 1, :, cs] = r[tok:]

            def rs(k, j, src, dst, dev):
                cp = remote(src, dst, rs_s.at[l, k, j], rs_r.at[l, k, j], dev)
                cp.start()
                pending_sends.append(cp)
                return cp

            def rs_pair(k):
                ds = pl.ds(*chunks[k])
                for ch in range(chips):
                    psend[l, ch, :, ds] = pf[2 * ch + 1 - c, :, ds].astype(BF16)
                return rs(k, 0, psend.at[l, :, :, ds], prx.at[l, :, :, ds], partner)

            def chip_sum(k, chip):
                ds = pl.ds(*chunks[k])
                return pf[2 * chip + c, :, ds] + prx[l, chip, :, ds].astype(F32)

            def rs_far(k, cp):
                ds = pl.ds(*chunks[k])
                cp.wait_recv()
                fsend[l, :, ds] = chip_sum(k, far_chip).astype(BF16)
                cp_far = rs(k, 1, fsend.at[l, :, ds], frx.at[l, :, ds], fwd)
                n1send[l, :, ds] = chip_sum(k, bwd_chip).astype(BF16)
                cp_n1 = rs(k, 2, n1send.at[l, :, ds], n1rx.at[l, :, ds], bwd)
                return cp_far, cp_n1

            def rs_near(k, cp_far):
                ds = pl.ds(*chunks[k])
                cp_far.wait_recv()
                n2send[l, :, ds] = (chip_sum(k, fwd_chip) + frx[l, :, ds].astype(F32)).astype(BF16)
                return rs(k, 3, n2send.at[l, :, ds], n2rx.at[l, :, ds], fwd)

            def rs_final(k, cp_n1, cp_n2):
                ds = pl.ds(*chunks[k])
                cp_n1.wait_recv()
                cp_n2.wait_recv()
                tot = (xres[:, ds].astype(F32) + chip_sum(k, xx) + n1rx[l, :, ds].astype(F32)
                       + n2rx[l, :, ds].astype(F32))
                return tot.astype(BF16)

            if l + 1 < layers:
                start_attn(l + 1)
            lax.fori_loop(0, n_b, step_b(0), 0)
            combine(0)
            cp_p0 = rs_pair(0)
            lax.fori_loop(0, n_b // 2, step_b(1), 0)
            cp_far0, cp_n10 = rs_far(0, cp_p0)
            lax.fori_loop(n_b // 2, n_b, step_b(1), 0)
            combine(1)
            cp_p1 = rs_pair(1)
            cp_n20 = rs_near(0, cp_far0)
            cp_far1, cp_n11 = rs_far(1, cp_p1)
            y0 = rs_final(0, cp_n10, cp_n20)
            cp_n21 = rs_near(1, cp_far1)
            y1 = rs_final(1, cp_n11, cp_n21)
            dst = out_ref if l + 1 == layers else xres
            dst[:, chunks[0][0]:chunks[0][0] + chunks[0][1]] = y0
            dst[:, chunks[1][0]:chunks[1][0] + chunks[1][1]] = y1

        for cp in pending_sends:
            cp.wait_send()

    vm = pltpu.VMEM
    cmax = max(cw for _, cw in chunks)
    nk = len(chunks)
    dma = pltpu.SemaphoreType.DMA
    scratch = [
        vm((d_model, heads * kv_dim), BF16), vm((heads * LATENT, d_model), BF16), vm((tok, seq, kv_dim), BF16),
        vm((NS, GA, d_model, ff), BF16), vm((NS, GA, d_model, ff), BF16), vm((n_b, GB, ff, cmax), BF16),
        vm((tok, d_model), BF16), vm((n_bg, heads * TB, kv_dim), BF16), vm((tok, heads * LATENT), BF16),
        vm((layers, group, tok, d_model), BF16), vm((group, layers * 2 * top_k, 2 * tok), F32),
        vm((n_rows, n_tok), BF16), vm((chips, 6 * tok, n_rows), BF16),
        vm((n_rows, d_model), BF16), vm((n_rows, ff), BF16),
        vm((n_tok, ff // group), BF16), vm((group, tok, d_model), F32),
        vm((layers, chips, tok, d_model), BF16), vm((layers, chips, tok, d_model), BF16),
        vm((layers, tok, d_model), BF16), vm((layers, tok, d_model), BF16),
        vm((layers, tok, d_model), BF16), vm((layers, tok, d_model), BF16),
        vm((layers, tok, d_model), BF16), vm((layers, tok, d_model), BF16),
        dma((heads // 2,)), dma((n_bg,)), dma, dma((2, NS)), dma((n_b,)),
        dma((group - 1,)), dma((group - 1,)), dma((layers, 7)), dma((layers, 7)),
        dma((layers, nk, 4)), dma((layers, nk, 4)),
    ]
    return kernel, scratch


def solution(mesh):
    group = mesh.shape['dp']
    tok_axes = ('replica', 'dp')
    in_specs = (
        P(tok_axes, None), P(tok_axes), P(None, tok_axes, None, None),
        P(None, None, None), P(None, None, None),
        P(None, tok_axes, None), P(None, tok_axes, None), P(None, tok_axes, None),
        P(None, 'dp', None, None), P(None, 'dp', None, None), P(None, 'dp', None, None),
        P(None, None, 'dp'), P(None, None, 'dp'), P(None, 'dp', None),
    )

    def device_step(x, lengths, cache, w_q, w_o, expert_ids, slots, route_w, w1_exp, w3_exp, w2_exp, w1_sh, w3_sh, w2_sh):
        tok, d_model = x.shape
        layers, _, seq, kv_dim = cache.shape
        heads = w_q.shape[2] // kv_dim
        n_exp, ff = w1_exp.shape[1], w1_exp.shape[3]
        top_k = expert_ids.shape[2]
        cap = max(1, (2 * tok * top_k) // (n_exp * group))
        me = lax.axis_index('dp')
        rows_e = group * cap
        code = jnp.where(slots >= 0, expert_ids * rows_e + me * cap + slots, DROPPED).astype(F32)
        tab = jnp.concatenate([code.transpose(0, 2, 1), route_w.transpose(0, 2, 1)], axis=1)
        tab = jnp.concatenate([tab, tab], axis=2).reshape(layers * 2 * top_k, 2 * tok)
        chunks = ((0, 512), (512, d_model - 512))
        kernel, scratch = make_kernel(group, layers, tok, d_model, seq, kv_dim, heads, n_exp, top_k, cap, ff, chunks)
        vmem = pl.BlockSpec(memory_space=pltpu.VMEM)
        hbm = pl.BlockSpec(memory_space=pl.ANY)
        return pl.pallas_call(
            kernel,
            name='mla_moe_decode',
            out_shape=jax.ShapeDtypeStruct((tok, d_model), BF16),
            in_specs=[vmem, pl.BlockSpec(memory_space=pltpu.SMEM), vmem, vmem, vmem, vmem] + [hbm] * 6,
            out_specs=vmem,
            scratch_shapes=scratch,
            compiler_params=pltpu.CompilerParams(collective_id=0, has_side_effects=True, vmem_limit_bytes=67043328),
        )(x, lengths, tab, w1_sh.transpose(0, 2, 1), w3_sh.transpose(0, 2, 1), w2_sh,
          cache, w_q, w_o, w1_exp, w3_exp, w2_exp)

    return jax.shard_map(device_step, mesh=mesh, in_specs=in_specs, out_specs=P(tok_axes, None), check_vma=False)
```
